32 devices in a mesh: dp: 4 (over y, x), expert: 4 (over z), mp: 2 (over core).
Axes of the slice: x: 2, y: 2, z: 4, core: 2. Of those that a mesh axis runs over, the one named last changes fastest.
Arguments:
- base_weights: bfloat16 [8, 2560, 3072], P('expert', None, 'mp'), may hold values from -6 to 6
- delta_blocks: bfloat16 [512, 128, 128], P(('dp', 'expert', 'mp')), may hold values from -4 to 4
- block_ids: int32 [512], P(('dp', 'expert', 'mp')), may hold values from 0 to 3839, as said below
- block_counts: int32 [256], P(('dp', 'expert', 'mp')), may hold values from 0 to 2, as said below
- owner_map: int32 [8], replicated, may hold values from 0 to 7, as said below
Outputs:
- merged_weights: bfloat16 [8, 2560, 3072], P('expert', None, 'mp')
The draws below stay inside these ranges and needn't reach their ends.
Inputs may be any that keep to these rules, and one draw needn't show every extreme that they name: A permutation: expert e is held in serving position owner_map[e], by the serving group owner_map[e] // 2. `block_ids`: every slot of device s for owner q, used or not, names a block (e * 20 + r) * 24 + c with owner_map[e] // 2 == q // 2 and c // 12 == q % 2. Names may repeat within and across devices. `block_counts`: at most 2 used slots from one device to one owner; in every draw some owner receives exactly 2 blocks from every device.
All inputs are finite; a program needn't handle non-finite values.
Results may differ from the reference program's by a relative error of at most 0.001.
Values may be sent and summed in bfloat16 or wider, within the bound.
A program may use at most 192 MiB of HBM per device.

```python
import jax
import jax.numpy as jnp
from jax import lax

BS = 128
DW = 2560
FF2 = 3072
EXP_DEV = 2
CAP = 2
E = 8
N_DEST = 8
RBW = 20
CB = 24
CBD = 12
N_MP = 2
DEVICES = 32


def serving_order(key):
    return jax.random.permutation(jax.random.fold_in(key, 11), E).astype(jnp.int32)


def draw_owner_map(key, part):
    return serving_order(key)


def draw_block_ids(key, part):
    order = serving_order(key)
    inverse = jnp.zeros((E,), jnp.int32).at[order].set(jnp.arange(E, dtype=jnp.int32))
    length = DEVICES * N_DEST * CAP
    slots = jnp.arange(length, dtype=jnp.int32)
    group = slots // CAP % N_DEST
    owner = group // N_MP
    column_part = group % N_MP
    within = jax.random.randint(jax.random.fold_in(key, 31), (length,), 0, EXP_DEV).astype(jnp.int32)
    expert = inverse[owner * EXP_DEV + within]
    row_pick = jax.random.randint(jax.random.fold_in(key, 32), (length,), 0, RBW).astype(jnp.int32)
    col_pick = jax.random.randint(jax.random.fold_in(key, 33), (length,), 0, CBD).astype(jnp.int32)
    column = column_part * CBD + col_pick
    return ((expert * RBW + row_pick) * CB + column).astype(jnp.int32)


def draw_block_counts(key, part):
    tiers = jax.random.randint(jax.random.fold_in(key, 21), (N_DEST,), 0, 4).astype(jnp.int32)
    fullest = jax.random.randint(jax.random.fold_in(key, 22), (), 0, N_DEST).astype(jnp.int32)
    tiers = jnp.where(jnp.arange(N_DEST, dtype=jnp.int32) == fullest, 0, tiers)
    limit = jnp.right_shift(jnp.int32(8), tiers)
    trials = jax.random.randint(jax.random.fold_in(key, 23), (DEVICES, N_DEST, CAP), 0, 8).astype(jnp.int32)
    counts = jnp.sum((trials < limit[None, :, None]).astype(jnp.int32), axis=2)
    return counts.reshape(DEVICES * N_DEST).astype(jnp.int32)


def steps_of(rng, shape, pieces, smallest, high):
    loudness, own = 1.0, jax.random.fold_in(rng, 6)
    for position, parts in pieces:
        heights = jnp.exp(jax.random.uniform(jax.random.fold_in(own, position), (parts,), jnp.float32, smallest / len(pieces), high / len(pieces)))
        loudness = loudness * jnp.repeat(heights, shape[position] // parts).reshape([-1 if axis == position else 1 for axis in range(len(shape))])
    return loudness


def gaussian(own_key, shape, width, bound, pieces=(), kind=jnp.bfloat16):
    entries = jax.random.normal(own_key, shape, jnp.float32) * width
    if len(pieces) > 0:
        entries = steps_of(own_key, shape, pieces, -0.22, 0.18) * entries
    return jnp.clip(entries, min=-bound, max=bound).astype(kind)


def setup_inputs(seed: int = 0) -> dict:
    key_of = jax.random.split(jax.random.key(seed), 6)
    return {
        "base_weights": gaussian(key_of[0], (E, DW, FF2), 1.0, 6.0, ((0, 4), (2, 2))),
        "delta_blocks": gaussian(key_of[1], (DEVICES * N_DEST * CAP, BS, BS), 0.5, 4.0, ((0, 32),)),
        "block_ids": draw_block_ids(jax.random.fold_in(key_of[5], 71), 0),
        "block_counts": draw_block_counts(jax.random.fold_in(key_of[5], 71), 0),
        "owner_map": draw_owner_map(jax.random.fold_in(key_of[5], 71), 0),
    }


def reference(base_weights, delta_blocks, block_ids, block_counts, owner_map):
    slot_count = N_DEST * CAP
    row_blocks = DW // BS
    col_total = FF2 // BS
    block_total = E * row_blocks * col_total
    listed = delta_blocks.reshape(DEVICES, slot_count, BS, BS)
    idents = block_ids.reshape(DEVICES, slot_count)
    counts = block_counts.reshape(DEVICES, N_DEST)
    active = (jnp.arange(slot_count, dtype=jnp.int32) % CAP)[None, :] < jnp.repeat(counts, CAP, axis=1)

    def add_source(running, record):
        values, names, usable = record
        values = jnp.where(usable[:, None, None], values.astype(jnp.float32), jnp.float32(0.0))
        return running.at[names].add(values), None

    start = jnp.zeros((block_total, BS, BS), jnp.float32)
    summed, unused = lax.scan(add_source, start, (listed, idents, active))
    grid = summed.reshape(E, row_blocks, col_total, BS, BS).transpose(0, 1, 3, 2, 4)
    task_delta = grid.reshape(E, DW, FF2)
    serving = jnp.zeros((E, DW, FF2), jnp.float32).at[owner_map].set(task_delta)
    return (base_weights.astype(jnp.float32) + serving).astype(jnp.bfloat16)
```

```python
import functools

import jax
import jax.numpy as jnp
from jax import lax
from jax.experimental import pallas as pl
from jax.experimental.pallas import tpu as pltpu
from jax.sharding import PartitionSpec as P

MESH = pl.DeviceIdType.MESH
LANES = 128


def flip(value, mask):
    bit = 1
    while bit <= mask:
        if mask & bit:
            value = value + bit - 2 * bit * (value // bit % 2)
        bit *= 2
    return value


def exchange_kernel(sizes, delta, names, got, got_names, local_sem, z_send, z_recv, x_send, x_recv,
                    y_send, y_recv, relay_send, relay_recv, name_send, name_recv):
    n_expert, n_mp = sizes
    n_dest = n_expert * n_mp
    d = lax.axis_index("dp")
    me = lax.axis_index("expert") * n_mp + lax.axis_index("mp")
    x_dp, y_dp = flip(d, 1), flip(d, 2)

    def column(k):
        g = flip(me, k)
        return g, (d, g // n_mp, g % n_mp)

    x_id = (x_dp, me // n_mp, me % n_mp)
    y_id = (y_dp, me // n_mp, me % n_mp)

    def remote(src, dst, send, recv, device):
        return pltpu.make_async_remote_copy(
            src_ref=src, dst_ref=dst, send_sem=send, recv_sem=recv, device_id=device, device_id_type=MESH
        )

    barrier = pltpu.get_barrier_semaphore()
    for k in range(1, n_dest):
        pl.semaphore_signal(barrier, inc=1, device_id=column(k)[1], device_id_type=MESH)
    pl.semaphore_signal(barrier, inc=1, device_id=x_id, device_id_type=MESH)
    pl.semaphore_signal(barrier, inc=1, device_id=y_id, device_id_type=MESH)
    own = pltpu.make_async_copy(delta.at[me], got.at[d, me], local_sem.at[0])
    own.start()
    own_names = pltpu.make_async_copy(names, got_names.at[d, me], local_sem.at[1])
    own_names.start()
    pl.semaphore_wait(barrier, n_dest + 1)

    sent = []
    to_x, to_y = [], []

    def to_neighbours(k):
        g = column(k)[0]
        src = delta.at[me] if k == 0 else got.at[d, g]
        for copies, send, recv, device in ((to_x, x_send, x_recv, x_id), (to_y, y_send, y_recv, y_id)):
            copy = remote(src, got.at[d, g], send.at[k], recv.at[k], device)
            copy.start()
            copies.append(copy)
            sent.append(copy)

    name_copies = []
    for k in range(1, n_dest):
        copy = remote(names, got_names.at[d, me], name_send.at[k], name_recv.at[k], column(k)[1])
        copy.start()
        name_copies.append(copy)
    sent.extend(name_copies)
    to_neighbours(0)
    z_copies = [None]
    for k in range(1, n_dest):
        g, device = column(k)
        copy = remote(delta.at[g], got.at[d, me], z_send.at[k], z_recv.at[k], device)
        copy.start()
        z_copies.append(copy)
        sent.append(copy)

    relays = []

    def relay(k):
        g = column(k)[0]
        if k % 2 == 0:
            to_x[k].wait_recv()
            part, device = got.at[x_dp, g], y_id
        else:
            to_y[k].wait_recv()
            part, device = got.at[y_dp, g], x_id
        copy = remote(part, part, relay_send.at[k], relay_recv.at[k], device)
        copy.start()
        relays.append(copy)
        sent.append(copy)

    lag = 2
    name_x = name_y = None
    for k in range(1, n_dest + lag):
        if k < n_dest:
            z_copies[k].wait_recv()
            to_neighbours(k)
        if k == 2:
            for copy in name_copies:
                copy.wait_recv()
            own_names.wait()
            mine = got_names.at[d]
            name_x = remote(mine, mine, name_send.at[n_dest], name_recv.at[n_dest], x_id)
            name_x.start()
            name_y = remote(mine, mine, name_send.at[n_dest + 1], name_recv.at[n_dest + 1], y_id)
            name_y.start()
        if k >= lag:
            relay(k - lag)
    name_x.wait_recv()
    theirs = got_names.at[x_dp]
    name_relay = remote(theirs, theirs, name_send.at[0], name_recv.at[0], y_id)
    name_relay.start()
    sent.extend([name_x, name_y, name_relay])

    for k in range(n_dest):
        (to_y if k % 2 == 0 else to_x)[k].wait_recv()
    for copy in relays:
        copy.wait_recv()
    name_y.wait_recv()
    name_relay.wait_recv()
    own.wait()
    for copy in sent:
        copy.wait_send()


def exchange(delta, names, sizes, n_dp):
    n_dest = delta.shape[0]
    moved = n_dp * delta.size * 2
    vmem = pl.BlockSpec(memory_space=pltpu.VMEM)
    dma = pltpu.SemaphoreType.DMA
    return pl.pallas_call(
        functools.partial(exchange_kernel, sizes),
        out_shape=(
            jax.ShapeDtypeStruct((n_dp,) + delta.shape, delta.dtype),
            jax.ShapeDtypeStruct((n_dp, n_dest) + names.shape, names.dtype),
        ),
        in_specs=[vmem, vmem],
        out_specs=(vmem, vmem),
        scratch_shapes=[dma((2,))] + [dma((n_dest,))] * 8 + [dma((n_dest + 2,))] * 2,
        compiler_params=pltpu.CompilerParams(
            collective_id=0, has_side_effects=True, vmem_limit_bytes=moved + moved // 4 + 4 * 1024 * 1024
        ),
        cost_estimate=pl.CostEstimate(flops=0, bytes_accessed=32 * moved, transcendentals=0),
    )(delta, names)


def apply_kernel(grid, names, got, base, out, table, listed, total, patch, base_sem, patch_sem):
    row_blocks, col_blocks, pieces = grid
    sources, capacity, size = got.shape[0], got.shape[1], got.shape[2]
    experts, rows, _ = base.shape
    me = lax.axis_index("expert") * lax.axis_size("mp") + lax.axis_index("mp")
    step = rows // pieces

    def base_copy(i):
        part = (i // pieces, pl.ds(i % pieces * step, step))
        return pltpu.make_async_copy(base.at[part], out.at[part], base_sem.at[i])

    for i in range(experts * pieces):
        base_copy(i).start()

    def clear(i, carry):
        table[i] = 0
        return carry

    lax.fori_loop(0, table.shape[0], clear, 0, unroll=16)

    def place(name):
        column = pl.multiple_of(name % col_blocks * size, size)
        row = pl.multiple_of(name // col_blocks % row_blocks * size, size)
        return name // (col_blocks * row_blocks), pl.ds(row, size), pl.ds(column, size)

    def add(slot, count):
        source, k = slot // capacity, slot % capacity
        name = names[source, me * capacity + k]
        live = name >= 0
        seen = table[jnp.maximum(name, 0)]
        fresh = jnp.logical_and(live, seen == 0)

        @pl.when(fresh)
        def _():
            table[name] = count + 1
            listed[count] = name
            total[count] = base[place(name)].astype(jnp.float32) + got[source, k].astype(jnp.float32)

        @pl.when(jnp.logical_and(live, seen > 0))
        def _():
            total[seen - 1] += got[source, k].astype(jnp.float32)

        return count + fresh.astype(jnp.int32)

    count = lax.fori_loop(0, sources * capacity, add, jnp.int32(0))

    def round_once(i, carry):
        patch[i] = total[i].astype(patch.dtype)
        return carry

    lax.fori_loop(0, count, round_once, 0)
    for i in range(experts * pieces):
        base_copy(i).wait()

    def patch_copy(i):
        return pltpu.make_async_copy(patch.at[i], out.at[place(listed[i])], patch_sem.at[i])

    def start(i, carry):
        patch_copy(i).start()
        return carry

    def finish(i, carry):
        patch_copy(i).wait()
        return carry

    lax.fori_loop(0, count, start, 0)
    lax.fori_loop(0, count, finish, 0)


def apply(names, got, base, row_blocks, col_blocks):
    experts = base.shape[0]
    size = got.shape[-1]
    blocks = experts * row_blocks * col_blocks
    most = min(blocks, got.shape[0] * got.shape[1])
    pieces = 4
    vmem = pl.BlockSpec(memory_space=pltpu.VMEM)
    return pl.pallas_call(
        functools.partial(apply_kernel, (row_blocks, col_blocks, pieces)),
        out_shape=jax.ShapeDtypeStruct(base.shape, base.dtype),
        in_specs=[pl.BlockSpec(memory_space=pltpu.SMEM), vmem, vmem],
        out_specs=pl.BlockSpec(memory_space=pl.ANY),
        scratch_shapes=[
            pltpu.SMEM((blocks,), jnp.int32),
            pltpu.SMEM((most,), jnp.int32),
            pltpu.VMEM((most, size, size), jnp.float32),
            pltpu.VMEM((most, size, size), base.dtype),
            pltpu.SemaphoreType.DMA((experts * pieces,)),
            pltpu.SemaphoreType.DMA((most,)),
        ],
        compiler_params=pltpu.CompilerParams(
            vmem_limit_bytes=base.size * 2 + got.size * 2 + most * size * size * 6 + 4 * 1024 * 1024
        ),
        cost_estimate=pl.CostEstimate(flops=0, bytes_accessed=base.size * 4, transcendentals=0),
    )(names, got, base)


def body(base_weights, delta_blocks, block_ids, block_counts, owner_map):
    exp_dev, row_count, col_count = base_weights.shape
    size = delta_blocks.shape[1]
    row_blocks, col_blocks = row_count // size, col_count // size
    n_dp, n_expert, n_mp = lax.axis_size("dp"), lax.axis_size("expert"), lax.axis_size("mp")
    n_dest = n_expert * n_mp
    col_total = col_blocks * n_mp
    slots = delta_blocks.shape[0]
    capacity = slots // n_dest
    active = jnp.arange(slots, dtype=jnp.int32) % capacity < jnp.repeat(block_counts, capacity)
    expert = block_ids // (row_blocks * col_total)
    row_index = block_ids // col_total % row_blocks
    matches = expert[:, None] == jnp.arange(owner_map.shape[0], dtype=jnp.int32)[None, :]
    position = jnp.sum(jnp.where(matches, owner_map[None, :], 0), axis=1)
    idents = (position % exp_dev * row_blocks + row_index) * col_blocks + block_ids % col_blocks
    idents = jnp.where(active, idents, -1)
    width = -(-slots // LANES) * LANES
    names = jnp.pad(idents, (0, width - slots), constant_values=-1).reshape(1, width)
    blocks = delta_blocks.reshape(n_dest, capacity, size, size)
    got, got_names = exchange(blocks, names, (n_expert, n_mp), n_dp)
    return apply(
        got_names.reshape(n_dp * n_dest, width),
        got.reshape(n_dp * n_dest, capacity, size, size),
        base_weights, row_blocks, col_blocks,
    )


def solution(mesh):
    in_specs = (
        P("expert", None, "mp"),
        P(("dp", "expert", "mp"), None, None),
        P(("dp", "expert", "mp")),
        P(("dp", "expert", "mp")),
        P(),
    )
    out_specs = P("expert", None, "mp")
    return jax.shard_map(body, mesh=mesh, in_specs=in_specs, out_specs=out_specs, check_vma=False)
```

```python
import functools

import jax
import jax.numpy as jnp
from jax import lax
from jax.experimental import pallas as pl
from jax.experimental.pallas import tpu as pltpu
from jax.sharding import PartitionSpec as P

MESH = pl.DeviceIdType.MESH
VMEM = 67043328
SLACK = 1024 * 1024


def flip(value, mask):
    bit = 1
    while bit <= mask:
        if mask & bit:
            value = value + bit - 2 * bit * (value // bit % 2)
        bit *= 2
    return value


def exchange_kernel(sizes, delta_in, ids_in, counts_in, owners, base_in, got, names, got_counts, base,
                    delta, own_ids, own_counts, got_ids, local_sem, base_sem, z_send, z_recv,
                    x_send, x_recv, y_send, y_recv, relay_send, relay_recv, ids_send, ids_recv,
                    counts_send, counts_recv):
    n_expert, n_mp, row_blocks, col_blocks = sizes
    n_dest = n_expert * n_mp
    d = lax.axis_index("dp")
    me = lax.axis_index("expert") * n_mp + lax.axis_index("mp")
    x_dp, y_dp = flip(d, 1), flip(d, 2)

    def column(k):
        g = flip(me, k)
        return g, (d, g // n_mp, g % n_mp)

    x_id = (x_dp, me // n_mp, me % n_mp)
    y_id = (y_dp, me // n_mp, me % n_mp)

    def remote(src, dst, send, recv, device):
        return pltpu.make_async_remote_copy(
            src_ref=src, dst_ref=dst, send_sem=send, recv_sem=recv, device_id=device, device_id_type=MESH
        )

    barrier = pltpu.get_barrier_semaphore()
    for k in range(1, n_dest):
        pl.semaphore_signal(barrier, inc=1, device_id=column(k)[1], device_id_type=MESH)
    pl.semaphore_signal(barrier, inc=1, device_id=x_id, device_id_type=MESH)
    pl.semaphore_signal(barrier, inc=1, device_id=y_id, device_id_type=MESH)
    early = [
        pltpu.make_async_copy(delta_in, delta, local_sem.at[0]),
        pltpu.make_async_copy(ids_in, own_ids, local_sem.at[1]),
        pltpu.make_async_copy(counts_in, own_counts, local_sem.at[2]),
    ]
    late = [
        pltpu.make_async_copy(delta_in.at[me], got.at[d, me], local_sem.at[3]),
        pltpu.make_async_copy(ids_in, got_ids.at[d, me], local_sem.at[4]),
        pltpu.make_async_copy(counts_in, got_counts.at[d, me], local_sem.at[5]),
    ]
    for copy in early + late:
        copy.start()
    for copy in early:
        copy.wait()
    pl.semaphore_wait(barrier, n_dest + 1)

    sent = []
    to_x, to_y = [], []

    def to_neighbours(k):
        g = column(k)[0]
        src = delta.at[me] if k == 0 else got.at[d, g]
        for copies, send, recv, device in ((to_x, x_send, x_recv, x_id), (to_y, y_send, y_recv, y_id)):
            copy = remote(src, got.at[d, g], send.at[k], recv.at[k], device)
            copy.start()
            copies.append(copy)
            sent.append(copy)

    small = ((own_ids, got_ids, ids_send, ids_recv), (own_counts, got_counts, counts_send, counts_recv))
    small_z, small_x, small_y, small_relay = [], [], [], []
    for k in range(1, n_dest):
        for own, all_of, send, recv in small:
            copy = remote(own, all_of.at[d, me], send.at[k], recv.at[k], column(k)[1])
            copy.start()
            small_z.append(copy)
    to_neighbours(0)
    z_copies = [None]
    for k in range(1, n_dest):
        g, device = column(k)
        copy = remote(delta.at[g], got.at[d, me], z_send.at[k], z_recv.at[k], device)
        copy.start()
        z_copies.append(copy)
        sent.append(copy)
    base_copies = [
        pltpu.make_async_copy(base_in.at[i], base.at[i], base_sem.at[i]) for i in range(base.shape[0])
    ]
    for copy in base_copies:
        copy.start()

    relays = []

    def relay(k):
        g = column(k)[0]
        if k % 2 == 0:
            to_x[k].wait_recv()
            part, device = got.at[x_dp, g], y_id
        else:
            to_y[k].wait_recv()
            part, device = got.at[y_dp, g], x_id
        copy = remote(part, part, relay_send.at[k], relay_recv.at[k], device)
        copy.start()
        relays.append(copy)
        sent.append(copy)

    lag = 2
    for k in range(1, n_dest + lag):
        if k < n_dest:
            z_copies[k].wait_recv()
            to_neighbours(k)
        if k == 2:
            for copy in small_z:
                copy.wait_recv()
            for copy in late[1:]:
                copy.wait()
            for own, all_of, send, recv in small:
                for copies, at, device in ((small_x, n_dest, x_id), (small_y, n_dest + 1, y_id)):
                    copy = remote(all_of.at[d], all_of.at[d], send.at[at], recv.at[at], device)
                    copy.start()
                    copies.append(copy)
        if k >= lag:
            relay(k - lag)
        if k == n_dest - 1:
            for (own, all_of, send, recv), arrived in zip(small, small_x):
                arrived.wait_recv()
                copy = remote(all_of.at[x_dp], all_of.at[x_dp], send.at[0], recv.at[0], y_id)
                copy.start()
                small_relay.append(copy)
    for copy in small_y + small_relay:
        copy.wait_recv()

    per_expert = row_blocks * col_blocks * n_mp
    exp_dev = base.shape[0]

    def whole_quotient(value, divisor):
        return ((value.astype(jnp.float32) + 0.5) * (1.0 / divisor)).astype(jnp.int32)

    def decode(i, carry):
        ids = got_ids[i // n_dest, i % n_dest]
        expert = whole_quotient(ids, per_expert)
        row = whole_quotient(ids, col_blocks * n_mp)
        column_block = ids - row * (col_blocks * n_mp)
        column_block -= whole_quotient(column_block, col_blocks) * col_blocks
        row -= expert * row_blocks
        place = jnp.zeros_like(ids)
        for e in range(owners.shape[0]):
            place = jnp.where(expert == e, owners[e], place)
        place -= whole_quotient(place, exp_dev) * exp_dev
        names[i // n_dest, i % n_dest] = (place * row_blocks + row) * col_blocks + column_block
        return carry

    lax.fori_loop(0, got_ids.shape[0] * n_dest, decode, 0)

    for k in range(n_dest):
        (to_y if k % 2 == 0 else to_x)[k].wait_recv()
    for copy in relays:
        copy.wait_recv()
    late[0].wait()
    for copy in base_copies:
        copy.wait()
    for copy in sent + small_z + small_x + small_y + small_relay:
        copy.wait_send()


def exchange(delta, ids, counts, owners, base, sizes, n_dp):
    n_dest = delta.shape[0]
    moved = n_dp * delta.size * 2
    vmem = pl.BlockSpec(memory_space=pltpu.VMEM)
    hbm = pl.BlockSpec(memory_space=pl.ANY)
    dma = pltpu.SemaphoreType.DMA
    return pl.pallas_call(
        functools.partial(exchange_kernel, sizes),
        out_shape=(
            pltpu.VMEM((n_dp,) + delta.shape, delta.dtype),
            pltpu.VMEM((n_dp, n_dest) + ids.shape, ids.dtype),
            pltpu.VMEM((n_dp, n_dest) + counts.shape, counts.dtype),
            pltpu.VMEM(base.shape, base.dtype),
        ),
        in_specs=[hbm, hbm, hbm, pl.BlockSpec(memory_space=pltpu.SMEM), hbm],
        out_specs=(vmem, vmem, vmem, vmem),
        scratch_shapes=[
            pltpu.VMEM(delta.shape, delta.dtype),
            pltpu.VMEM(ids.shape, ids.dtype),
            pltpu.VMEM(counts.shape, counts.dtype),
            pltpu.VMEM((n_dp, n_dest) + ids.shape, ids.dtype),
            dma((6,)),
            dma((base.shape[0],)),
        ] + [dma((n_dest,))] * 8 + [dma((n_dest + 2,))] * 4,
        compiler_params=pltpu.CompilerParams(
            collective_id=0, has_side_effects=True, vmem_limit_bytes=VMEM - moved - base.size * 2 - SLACK
        ),
        cost_estimate=pl.CostEstimate(flops=0, bytes_accessed=32 * moved, transcendentals=0),
    )(delta, ids, counts, owners, base)


def apply_kernel(grid, names, counts, got, base_in, out, base, table, link, listed, listed_count, patch,
                 base_sem, patch_sem):
    row_blocks, col_blocks, pieces = grid
    sources, capacity, size = got.shape[0], got.shape[1], got.shape[2]
    experts, rows, _ = base.shape
    per_expert = row_blocks * col_blocks
    most = patch.shape[0]
    me = lax.axis_index("expert") * lax.axis_size("mp") + lax.axis_index("mp")
    step = rows // pieces
    split = experts // 2
    scale = -(-(1 << 16) // col_blocks)
    assert per_expert * (scale * col_blocks - (1 << 16)) < 1 << 16

    def base_copy(e, i):
        part = (e, pl.ds(i * step, step))
        return pltpu.make_async_copy(base.at[part], out.at[part], base_sem.at[e * pieces + i])

    def each_base_copy(first, last, action):
        for e in range(first, last):
            for i in range(pieces):
                action(base_copy(e, i))

    each_base_copy(0, split, lambda copy: copy.start())

    def clear(i, carry):
        table[i] = 0
        return carry

    lax.fori_loop(0, table.shape[0], clear, 0, unroll=16)
    for e in range(experts):
        listed_count[e] = 0

    def enter(slot, source, k):
        name = names[source, 0, me * capacity + k]

        @pl.when(k < counts[source, 0, me])
        def _():
            before = table[name]
            table[name] = slot + 1
            link[slot] = before

            @pl.when(before == 0)
            def _():
                e = jnp.int32(0)
                for other in range(1, experts):
                    e += (name >= other * per_expert).astype(jnp.int32)
                count = listed_count[e]
                listed[e * most + count] = name
                listed_count[e] = count + 1

    def enter_source(source, carry):
        for k in range(capacity):
            enter(source * capacity + k, source, k)
        return carry

    lax.fori_loop(0, sources, enter_source, 0)

    def place(e, name):
        rest = name - e * per_expert
        row = lax.shift_right_logical(rest * scale, 16)
        column = rest - row * col_blocks
        return (
            e,
            pl.ds(pl.multiple_of(row * size, size), size),
            pl.ds(pl.multiple_of(column * size, size), size),
        )

    def block_of(slot):
        return got[slot // capacity, slot % capacity].astype(jnp.float32)

    def summed(name, spot):
        head = table[name] - 1
        total = base[spot].astype(jnp.float32) + block_of(head)
        _, total = lax.while_loop(
            lambda state: state[0] > 0,
            lambda state: (link[state[0] - 1], state[1] + block_of(state[0] - 1)),
            (link[head], total),
        )
        return total.astype(base.dtype)

    for e in range(split, experts):
        def in_place(i, carry, e=e):
            name = listed[e * most + i]
            spot = place(e, name)
            base[spot] = summed(name, spot)
            return carry

        lax.fori_loop(0, listed_count[e], in_place, 0)
    each_base_copy(split, experts, lambda copy: copy.start())

    def patch_copy(e, i, at):
        return pltpu.make_async_copy(patch.at[at], out.at[place(e, listed[e * most + i])], patch_sem.at[at])

    first = jnp.int32(0)
    starts = []
    for e in range(split):
        starts.append(first)

        def aside(i, carry, e=e, first=first):
            name = listed[e * most + i]
            patch[first + i] = summed(name, place(e, name))
            return carry

        lax.fori_loop(0, listed_count[e], aside, 0)
        first = first + listed_count[e]
    each_base_copy(0, split, lambda copy: copy.wait())
    for e, first in enumerate(starts):
        def start(i, carry, e=e, first=first):
            patch_copy(e, i, first + i).start()
            return carry

        lax.fori_loop(0, listed_count[e], start, 0)
    each_base_copy(split, experts, lambda copy: copy.wait())
    for e, first in enumerate(starts):
        def finish(i, carry, e=e, first=first):
            patch_copy(e, i, first + i).wait()
            return carry

        lax.fori_loop(0, listed_count[e], finish, 0)


def apply(names, counts, got, base, row_blocks, col_blocks):
    experts = base.shape[0]
    size = got.shape[-1]
    blocks = experts * row_blocks * col_blocks
    slots = got.shape[0] * got.shape[1]
    most = min(blocks, slots)
    pieces = 4
    vmem = pl.BlockSpec(memory_space=pltpu.VMEM)
    smem = pl.BlockSpec(memory_space=pltpu.SMEM)
    out, _ = pl.pallas_call(
        functools.partial(apply_kernel, (row_blocks, col_blocks, pieces)),
        out_shape=(
            jax.ShapeDtypeStruct(base.shape, base.dtype),
            jax.ShapeDtypeStruct(base.shape, base.dtype),
        ),
        in_specs=[smem, smem, vmem, vmem],
        out_specs=(pl.BlockSpec(memory_space=pl.ANY), vmem),
        input_output_aliases={3: 1},
        scratch_shapes=[
            pltpu.SMEM((blocks,), jnp.int32),
            pltpu.SMEM((slots,), jnp.int32),
            pltpu.SMEM((experts * most,), jnp.int32),
            pltpu.SMEM((experts,), jnp.int32),
            pltpu.VMEM((most, size, size), base.dtype),
            pltpu.SemaphoreType.DMA((experts * pieces,)),
            pltpu.SemaphoreType.DMA((most,)),
        ],
        compiler_params=pltpu.CompilerParams(vmem_limit_bytes=most * size * size * 2 + 4 * 1024 * 1024),
        cost_estimate=pl.CostEstimate(flops=0, bytes_accessed=base.size * 4, transcendentals=0),
    )(names, counts, got, base)
    return out


def body(base_weights, delta_blocks, block_ids, block_counts, owner_map):
    exp_dev, row_count, col_count = base_weights.shape
    size = delta_blocks.shape[1]
    row_blocks, col_blocks = row_count // size, col_count // size
    n_dp, n_expert, n_mp = lax.axis_size("dp"), lax.axis_size("expert"), lax.axis_size("mp")
    n_dest = n_expert * n_mp
    slots = delta_blocks.shape[0]
    capacity = slots // n_dest
    assert owner_map.shape[0] * row_blocks * col_blocks * n_mp < 1 << 20
    sources = n_dp * n_dest
    got, names, counts, base = exchange(
        delta_blocks.reshape(n_dest, capacity, size, size),
        block_ids.reshape(1, slots),
        block_counts.reshape(1, n_dest),
        owner_map, base_weights, (n_expert, n_mp, row_blocks, col_blocks), n_dp,
    )
    return apply(
        names.reshape(sources, 1, slots),
        counts.reshape(sources, 1, n_dest),
        got.reshape(sources, capacity, size, size),
        base, row_blocks, col_blocks,
    )


def solution(mesh):
    in_specs = (
        P("expert", None, "mp"),
        P(("dp", "expert", "mp"), None, None),
        P(("dp", "expert", "mp")),
        P(("dp", "expert", "mp")),
        P(),
    )
    out_specs = P("expert", None, "mp")
    return jax.shard_map(body, mesh=mesh, in_specs=in_specs, out_specs=out_specs, check_vma=False)
```

```python
import functools

import jax
import jax.numpy as jnp
from jax import lax
from jax.experimental import pallas as pl
from jax.experimental.pallas import tpu as pltpu
from jax.sharding import PartitionSpec as P

MESH = pl.DeviceIdType.MESH
VMEM = 67043328
SLACK = 1024 * 1024


def flip(value, mask):
    bit = 1
    while bit <= mask:
        if mask & bit:
            value = value + bit - 2 * bit * (value // bit % 2)
        bit *= 2
    return value


def exchange_kernel(sizes, delta_in, ids_in, counts_in, owners, base_in, got, names, got_counts, base,
                    delta, own_ids, own_counts, got_ids, local_sem, base_sem, z_send, z_recv,
                    x_send, x_recv, y_send, y_recv, relay_send, relay_recv, ids_send, ids_recv,
                    counts_send, counts_recv):
    n_expert, n_mp, row_blocks, col_blocks = sizes
    n_dest = n_expert * n_mp
    d = lax.axis_index("dp")
    me = lax.axis_index("expert") * n_mp + lax.axis_index("mp")
    x_dp, y_dp = flip(d, 1), flip(d, 2)

    def column(k):
        g = flip(me, k)
        return g, (d, g // n_mp, g % n_mp)

    x_id = (x_dp, me // n_mp, me % n_mp)
    y_id = (y_dp, me // n_mp, me % n_mp)

    def remote(src, dst, send, recv, device):
        return pltpu.make_async_remote_copy(
            src_ref=src, dst_ref=dst, send_sem=send, recv_sem=recv, device_id=device, device_id_type=MESH
        )

    barrier = pltpu.get_barrier_semaphore()
    for k in range(1, n_dest):
        pl.semaphore_signal(barrier, inc=1, device_id=column(k)[1], device_id_type=MESH)
    pl.semaphore_signal(barrier, inc=1, device_id=x_id, device_id_type=MESH)
    pl.semaphore_signal(barrier, inc=1, device_id=y_id, device_id_type=MESH)
    early = [
        pltpu.make_async_copy(delta_in, delta, local_sem.at[0]),
        pltpu.make_async_copy(ids_in, own_ids, local_sem.at[1]),
        pltpu.make_async_copy(counts_in, own_counts, local_sem.at[2]),
    ]
    late = [
        pltpu.make_async_copy(delta_in.at[me], got.at[d, me], local_sem.at[3]),
        pltpu.make_async_copy(ids_in, got_ids.at[d, me], local_sem.at[4]),
        pltpu.make_async_copy(counts_in, got_counts.at[d, me], local_sem.at[5]),
    ]
    for copy in early + late:
        copy.start()
    for copy in early:
        copy.wait()
    pl.semaphore_wait(barrier, n_dest + 1)

    sent = []
    to_x, to_y = [], []

    def to_neighbours(k):
        g = column(k)[0]
        src = delta.at[me] if k == 0 else got.at[d, g]
        for copies, send, recv, device in ((to_x, x_send, x_recv, x_id), (to_y, y_send, y_recv, y_id)):
            copy = remote(src, got.at[d, g], send.at[k], recv.at[k], device)
            copy.start()
            copies.append(copy)
            sent.append(copy)

    small = ((own_ids, got_ids, ids_send, ids_recv), (own_counts, got_counts, counts_send, counts_recv))
    small_z, small_x, small_y, small_relay = [], [], [], []
    for k in range(1, n_dest):
        for own, all_of, send, recv in small:
            copy = remote(own, all_of.at[d, me], send.at[k], recv.at[k], column(k)[1])
            copy.start()
            small_z.append(copy)
    to_neighbours(0)
    z_copies = [None]
    for k in range(1, n_dest):
        g, device = column(k)
        copy = remote(delta.at[g], got.at[d, me], z_send.at[k], z_recv.at[k], device)
        copy.start()
        z_copies.append(copy)
        sent.append(copy)
    base_copies = [
        pltpu.make_async_copy(base_in.at[i], base.at[i], base_sem.at[i]) for i in range(base.shape[0])
    ]
    for copy in base_copies:
        copy.start()

    relays = []

    def relay(k):
        g = column(k)[0]
        if k % 2 == 0:
            to_x[k].wait_recv()
            part, device = got.at[x_dp, g], y_id
        else:
            to_y[k].wait_recv()
            part, device = got.at[y_dp, g], x_id
        copy = remote(part, part, relay_send.at[k], relay_recv.at[k], device)
        copy.start()
        relays.append(copy)
        sent.append(copy)

    lag = 2
    for k in range(1, n_dest + lag):
        if k < n_dest:
            z_copies[k].wait_recv()
            to_neighbours(k)
        if k == 2:
            for copy in small_z:
                copy.wait_recv()
            for copy in late[1:]:
                copy.wait()
            for own, all_of, send, recv in small:
                for copies, at, device in ((small_x, n_dest, x_id), (small_y, n_dest + 1, y_id)):
                    copy = remote(all_of.at[d], all_of.at[d], send.at[at], recv.at[at], device)
                    copy.start()
                    copies.append(copy)
        if k >= lag:
            relay(k - lag)
        if k == n_dest - 1:
            for (own, all_of, send, recv), arrived in zip(small, small_x):
                arrived.wait_recv()
                copy = remote(all_of.at[x_dp], all_of.at[x_dp], send.at[0], recv.at[0], y_id)
                copy.start()
                small_relay.append(copy)
    for copy in small_y + small_relay:
        copy.wait_recv()

    per_expert = row_blocks * col_blocks * n_mp
    exp_dev = base.shape[0]

    def whole_quotient(value, divisor):
        return ((value.astype(jnp.float32) + 0.5) * (1.0 / divisor)).astype(jnp.int32)

    def decode(i, carry):
        ids = got_ids[i // n_dest, i % n_dest]
        expert = whole_quotient(ids, per_expert)
        row = whole_quotient(ids, col_blocks * n_mp)
        column_block = ids - row * (col_blocks * n_mp)
        column_block -= whole_quotient(column_block, col_blocks) * col_blocks
        row -= expert * row_blocks
        place = jnp.zeros_like(ids)
        for e in range(owners.shape[0]):
            place = jnp.where(expert == e, owners[e], place)
        place -= whole_quotient(place, exp_dev) * exp_dev
        names[i // n_dest, i % n_dest] = (place * row_blocks + row) * col_blocks + column_block
        return carry

    lax.fori_loop(0, got_ids.shape[0] * n_dest, decode, 0)

    for k in range(n_dest):
        (to_y if k % 2 == 0 else to_x)[k].wait_recv()
    for copy in relays:
        copy.wait_recv()
    late[0].wait()
    for copy in base_copies:
        copy.wait()
    for copy in sent + small_z + small_x + small_y + small_relay:
        copy.wait_send()


def exchange(delta, ids, counts, owners, base, sizes, n_dp):
    n_dest = delta.shape[0]
    moved = n_dp * delta.size * 2
    vmem = pl.BlockSpec(memory_space=pltpu.VMEM)
    hbm = pl.BlockSpec(memory_space=pl.ANY)
    dma = pltpu.SemaphoreType.DMA
    return pl.pallas_call(
        functools.partial(exchange_kernel, sizes),
        out_shape=(
            pltpu.VMEM((n_dp,) + delta.shape, delta.dtype),
            pltpu.VMEM((n_dp, n_dest) + ids.shape, ids.dtype),
            pltpu.VMEM((n_dp, n_dest) + counts.shape, counts.dtype),
            pltpu.VMEM(base.shape, base.dtype),
        ),
        in_specs=[hbm, hbm, hbm, pl.BlockSpec(memory_space=pltpu.SMEM), hbm],
        out_specs=(vmem, vmem, vmem, vmem),
        scratch_shapes=[
            pltpu.VMEM(delta.shape, delta.dtype),
            pltpu.VMEM(ids.shape, ids.dtype),
            pltpu.VMEM(counts.shape, counts.dtype),
            pltpu.VMEM((n_dp, n_dest) + ids.shape, ids.dtype),
            dma((6,)),
            dma((base.shape[0],)),
        ] + [dma((n_dest,))] * 8 + [dma((n_dest + 2,))] * 4,
        compiler_params=pltpu.CompilerParams(
            collective_id=0, has_side_effects=True, vmem_limit_bytes=VMEM - moved - base.size * 2 - SLACK
        ),
        cost_estimate=pl.CostEstimate(flops=0, bytes_accessed=32 * moved, transcendentals=0),
    )(delta, ids, counts, owners, base)


def apply_kernel(grid, names_in, counts_in, got, base_in, out, base, names, counts, table, link, listed,
                 listed_inside, patch, base_sem, patch_sem, local_sem):
    row_blocks, col_blocks, pieces, beside = grid
    sources, capacity, size = got.shape[0], got.shape[1], got.shape[2]
    experts, rows, _ = base.shape
    per_expert = row_blocks * col_blocks
    me = lax.axis_index("expert") * lax.axis_size("mp") + lax.axis_index("mp")
    step = rows // pieces
    border = beside * (row_blocks // pieces) * col_blocks
    scale = -(-(1 << 16) // col_blocks)
    assert per_expert * (scale * col_blocks - (1 << 16)) < 1 << 16

    def base_copy(i):
        part = (i // pieces, pl.ds(i % pieces * step, step))
        return pltpu.make_async_copy(base.at[part], out.at[part], base_sem.at[i])

    to_smem = [
        pltpu.make_async_copy(names_in, names, local_sem.at[0]),
        pltpu.make_async_copy(counts_in, counts, local_sem.at[1]),
    ]
    for copy in to_smem:
        copy.start()
    for i in range(beside):
        base_copy(i).start()

    def clear(i, carry):
        table[i] = 0
        return carry

    lax.fori_loop(0, table.shape[0], clear, 0, unroll=16)
    for copy in to_smem:
        copy.wait()

    def enter_source(source, carry):
        outside, inside = carry
        used = counts[source, 0, me]
        for k in range(capacity):
            slot = source * capacity + k
            name = names[source, 0, me * capacity + k]
            live = k < used
            before = table[name]
            link[slot] = before
            table[name] = jnp.where(live, slot + 1, before)
            listed[outside] = name
            listed_inside[inside] = name
            fresh = jnp.logical_and(live, before == 0).astype(jnp.int32)
            first_part = (name < border).astype(jnp.int32)
            outside, inside = outside + fresh * first_part, inside + fresh * (1 - first_part)
        return outside, inside

    outside, inside = lax.fori_loop(0, sources, enter_source, (jnp.int32(0), jnp.int32(0)))

    def place(name):
        e = jnp.int32(0)
        for other in range(1, experts):
            e += (name >= other * per_expert).astype(jnp.int32)
        rest = name - e * per_expert
        row = lax.shift_right_logical(rest * scale, 16)
        column = rest - row * col_blocks
        return (
            e,
            pl.ds(pl.multiple_of(row * size, size), size),
            pl.ds(pl.multiple_of(column * size, size), size),
        )

    def block_of(slot):
        return got[slot // capacity, slot % capacity].astype(jnp.float32)

    def summed(name, spot):
        head = table[name] - 1
        total = base[spot].astype(jnp.float32) + block_of(head)
        _, total = lax.while_loop(
            lambda state: state[0] > 0,
            lambda state: (link[state[0] - 1], state[1] + block_of(state[0] - 1)),
            (link[head], total),
        )
        return total.astype(base.dtype)

    def in_place(i, carry):
        spot = place(listed_inside[i])
        base[spot] = summed(listed_inside[i], spot)
        return carry

    lax.fori_loop(0, inside, in_place, 0)
    for i in range(beside, experts * pieces):
        base_copy(i).start()

    def aside(i, carry):
        patch[i] = summed(listed[i], place(listed[i]))
        return carry

    lax.fori_loop(0, outside, aside, 0)
    for i in range(beside):
        base_copy(i).wait()

    def patch_copy(i):
        return pltpu.make_async_copy(patch.at[i], out.at[place(listed[i])], patch_sem.at[i])

    def start(i, carry):
        patch_copy(i).start()
        return carry

    def finish(i, carry):
        patch_copy(i).wait()
        return carry

    lax.fori_loop(0, outside, start, 0)
    for i in range(beside, experts * pieces):
        base_copy(i).wait()
    lax.fori_loop(0, outside, finish, 0)


def apply(names, counts, got, base, row_blocks, col_blocks):
    experts = base.shape[0]
    size = got.shape[-1]
    blocks = experts * row_blocks * col_blocks
    slots = got.shape[0] * got.shape[1]
    most = min(blocks, slots)
    pieces = 4 if row_blocks % 4 == 0 else 1
    beside = experts * pieces * 5 // 8
    vmem = pl.BlockSpec(memory_space=pltpu.VMEM)
    out, _ = pl.pallas_call(
        functools.partial(apply_kernel, (row_blocks, col_blocks, pieces, beside)),
        out_shape=(
            jax.ShapeDtypeStruct(base.shape, base.dtype),
            jax.ShapeDtypeStruct(base.shape, base.dtype),
        ),
        in_specs=[vmem, vmem, vmem, vmem],
        out_specs=(pl.BlockSpec(memory_space=pl.ANY), vmem),
        input_output_aliases={3: 1},
        scratch_shapes=[
            pltpu.SMEM(names.shape, jnp.int32),
            pltpu.SMEM(counts.shape, jnp.int32),
            pltpu.SMEM((blocks,), jnp.int32),
            pltpu.SMEM((slots,), jnp.int32),
            pltpu.SMEM((most + 1,), jnp.int32),
            pltpu.SMEM((most + 1,), jnp.int32),
            pltpu.VMEM((most, size, size), base.dtype),
            pltpu.SemaphoreType.DMA((experts * pieces,)),
            pltpu.SemaphoreType.DMA((most,)),
            pltpu.SemaphoreType.DMA((2,)),
        ],
        compiler_params=pltpu.CompilerParams(vmem_limit_bytes=most * size * size * 2 + 4 * 1024 * 1024),
        cost_estimate=pl.CostEstimate(flops=0, bytes_accessed=base.size * 4, transcendentals=0),
    )(names, counts, got, base)
    return out


def body(base_weights, delta_blocks, block_ids, block_counts, owner_map):
    exp_dev, row_count, col_count = base_weights.shape
    size = delta_blocks.shape[1]
    row_blocks, col_blocks = row_count // size, col_count // size
    n_dp, n_expert, n_mp = lax.axis_size("dp"), lax.axis_size("expert"), lax.axis_size("mp")
    n_dest = n_expert * n_mp
    slots = delta_blocks.shape[0]
    capacity = slots // n_dest
    assert owner_map.shape[0] * row_blocks * col_blocks * n_mp < 1 << 20
    sources = n_dp * n_dest
    got, names, counts, base = exchange(
        delta_blocks.reshape(n_dest, capacity, size, size),
        block_ids.reshape(1, slots),
        block_counts.reshape(1, n_dest),
        owner_map, base_weights, (n_expert, n_mp, row_blocks, col_blocks), n_dp,
    )
    return apply(
        names.reshape(sources, 1, slots),
        counts.reshape(sources, 1, n_dest),
        got.reshape(sources, capacity, size, size),
        base, row_blocks, col_blocks,
    )


def solution(mesh):
    in_specs = (
        P("expert", None, "mp"),
        P(("dp", "expert", "mp"), None, None),
        P(("dp", "expert", "mp")),
        P(("dp", "expert", "mp")),
        P(),
    )
    out_specs = P("expert", None, "mp")
    return jax.shard_map(body, mesh=mesh, in_specs=in_specs, out_specs=out_specs, check_vma=False)
```
